32 devices in a mesh: tp: 8 (over z, core), fs: 4 (over y, x).
Axes of the slice: x: 2, y: 2, z: 4, core: 2. Of those that a mesh axis runs over, the one named last changes fastest.
Arguments:
- tokens: bfloat16 [128, 8192], P(('tp', 'fs')), may hold values from -6 to 6
- gate_weight: bfloat16 [8192, 29568], P('fs', 'tp'), may hold values from -0.0625 to 0.0625
- up_weight: bfloat16 [8192, 29568], P('fs', 'tp'), may hold values from -0.0625 to 0.0625
- down_weight: bfloat16 [29568, 8192], P('tp', 'fs'), may hold values from -0.046875 to 0.046875
Outputs:
- mixed: bfloat16 [128, 8192], P(None, ('fs', 'tp'))
The draws below stay inside these ranges and needn't reach their ends.
All inputs are finite; a program needn't handle non-finite values.
Results may differ from the reference program's by a relative error of at most 0.0049.
Values may be sent and summed in bfloat16 or wider, within the bound.
A program may use at most 128 MiB of HBM per device.

```python
import jax
import jax.numpy as jnp

D = 8192
FF = 29568
TOKENS = 128


def strengthened(values, key, source, target, shards_of, factor):
    owner, partner = [(jnp.arange(values.shape[dim]) // (values.shape[dim] // shards_of)).reshape([-1 if axis == dim else 1 for axis in range(values.ndim)]) for dim in (source, target)]
    chosen = jax.random.permutation(key, shards_of)[partner]
    strong = (owner == chosen) | (owner == (partner + shards_of // 2) % shards_of)
    return jnp.where(strong, factor * values, values)


def shard_levels(own_key, shape, pieces, low, high):
    def one(dim, blocks):
        draws = jax.random.uniform(jax.random.fold_in(jax.random.fold_in(own_key, 6), dim), (blocks,), jnp.float32, low / len(pieces), high / len(pieces))
        return jnp.repeat(jnp.exp(draws), shape[dim] // blocks).reshape((-1,) + (1,) * (len(shape) - dim - 1))

    level = one(*pieces[0])
    for cut in pieces[1:]:
        level = level * one(*cut)
    return level


def bell_draw(own_key, extent, spread, bound, pieces=(), held_as=jnp.bfloat16):
    loudness = shard_levels(own_key, extent, pieces, -0.22, 0.18) if pieces else 1.0
    entries = jax.random.normal(own_key, extent, jnp.float32) * spread * loudness
    return jnp.minimum(jnp.maximum(entries, -bound), bound).astype(held_as)


def gaussian_with(own_key, shape, width, most, split, heavy, kind=jnp.bfloat16):
    array = width * jax.random.normal(own_key, shape, jnp.float32)
    if split:
        array = array * shard_levels(own_key, shape, split, -0.22, 0.18)
    return jnp.clip(strengthened(array, jax.random.fold_in(own_key, 3), *heavy), -most, most).astype(kind)


def setup_inputs(seed: int = 0) -> dict:
    key_list = jax.random.split(jax.random.key(seed), 5)
    tokens = bell_draw(key_list[0], (TOKENS, D), 1.0, 6.0, ((0, 32),))
    gate_weight = bell_draw(key_list[1], (D, FF), D ** -0.5, 0.0625, ((0, 4), (1, 8)))
    up_weight = bell_draw(key_list[2], (D, FF), D ** -0.5, 0.0625, ((0, 4), (1, 8)))
    down_weight = gaussian_with(key_list[3], (FF, D), FF ** -0.5, 0.046875, ((0, 8), (1, 4)), (0, 1, 8, 2.0))
    return dict(tokens=tokens, gate_weight=gate_weight, up_weight=up_weight, down_weight=down_weight)


def reference(tokens, gate_weight, up_weight, down_weight):
    gate = jnp.dot(tokens, gate_weight, preferred_element_type=jnp.float32)
    up = jnp.dot(tokens, up_weight, preferred_element_type=jnp.float32)
    hidden = (jax.nn.silu(gate) * up).astype(jnp.bfloat16)
    mixed = jnp.dot(hidden, down_weight, preferred_element_type=jnp.float32)
    return mixed.astype(jnp.bfloat16)
```

```python
import jax
import jax.numpy as jnp
from jax import lax
from jax.sharding import PartitionSpec as P


def body(tokens, gate_weight, up_weight, down_weight):
    by_feature = lax.all_to_all(tokens, "fs", split_axis=1, concat_axis=0, tiled=True)
    feature_rows = lax.all_gather(by_feature, "tp", axis=0, tiled=True)
    gate_part = jnp.dot(feature_rows, gate_weight, preferred_element_type=jnp.float32)
    up_part = jnp.dot(feature_rows, up_weight, preferred_element_type=jnp.float32)
    gate, up = (
        lax.psum_scatter(gate_part, "fs", scatter_dimension=1, tiled=True),
        lax.psum_scatter(up_part, "fs", scatter_dimension=1, tiled=True),
    )
    hidden = (jax.nn.silu(gate) * up).astype(jnp.bfloat16)
    hidden_all = lax.all_gather(hidden, "fs", axis=1, tiled=True)
    partial_out = jnp.dot(hidden_all, down_weight, preferred_element_type=jnp.float32)
    summed = lax.psum_scatter(partial_out, "tp", scatter_dimension=1, tiled=True)
    return summed.astype(jnp.bfloat16)


def solution(mesh):
    return jax.shard_map(
        body,
        mesh=mesh,
        in_specs=(P(("tp", "fs"), None), P("fs", "tp"), P("fs", "tp"), P("tp", "fs")),
        out_specs=P(None, ("fs", "tp")),
        check_vma=False,
    )
```

```python
import functools

import jax
import jax.numpy as jnp
from jax import lax
from jax.experimental import pallas as pl
from jax.experimental.pallas import tpu as pltpu
from jax.sharding import PartitionSpec as P

BF16, F32 = jnp.bfloat16, jnp.float32
LANES, SUBLANES = 128, 16
CHUNK = 5 * LANES
LOADS = 4


def chunks_of(width):
    return [(at, min(CHUNK, width - at)) for at in range(0, width, CHUNK)]


def round_up(n, m):
    return (n + m - 1) // m * m


def kernel(n_tensor, n_stored, pieces, tok_ref, gate_hbm, up_hbm, down_hbm, out_ref,
           gate_w, up_w, down_w, blocks, x, part, own, rs_send, rs_recv, hid,
           acc, keep, pair_send, pair_recv, z_send, z_recv,
           load_sem, a_send, a_recv, b_send, b_recv, c_send, c_recv,
           rs_ssem, rs_rsem, ag_ssem, ag_rsem, p_ssem, p_rsem, z_ssem, z_rsem):
    tp, fs = lax.axis_index("tp"), lax.axis_index("fs")
    core, chip = lax.rem(tp, 2), tp // 2
    partner = tp + 1 - 2 * core
    n_chips = n_tensor // 2
    width = gate_w.shape[1]
    chunks = chunks_of(width)
    rows = own.shape[2]
    total = rows * n_stored
    lane_w = keep.shape[2]

    loads = []
    for i, (hbm, vmem) in enumerate(((gate_hbm, gate_w), (up_hbm, up_w), (down_hbm, down_w))):
        depth = hbm.shape[0]
        step = round_up((depth + LOADS - 1) // LOADS, SUBLANES)
        for j, at in enumerate(range(0, depth, step)):
            span = pl.ds(at, min(step, depth - at))
            copy = pltpu.make_async_copy(hbm.at[span, :], vmem.at[span, :], load_sem.at[i, j])
            copy.start()
            loads.append((i, copy))

    def remote(src, dst, ssem, rsem, tensor, stored):
        return pltpu.make_async_remote_copy(
            src_ref=src, dst_ref=dst, send_sem=ssem, recv_sem=rsem,
            device_id={"tp": tensor, "fs": stored},
            device_id_type=pl.DeviceIdType.MESH)

    others = [lax.rem(fs + j, n_stored) for j in range(1, n_stored)]
    sources = [lax.rem(fs + n_stored - j, n_stored) for j in range(1, n_stored)]
    chips = [lax.rem(chip + j, n_chips) for j in range(1, n_chips)]
    chip_sources = [lax.rem(chip + n_chips - j, n_chips) for j in range(1, n_chips)]

    barrier = pltpu.get_barrier_semaphore()
    peers = [(tp, f) for f in others] + [(2 * d + core, fs) for d in chips] + [(partner, fs)]
    for tensor, stored in peers:
        pl.semaphore_signal(barrier, inc=1, device_id={"tp": tensor, "fs": stored},
                            device_id_type=pl.DeviceIdType.MESH)
    blocks[tp, fs] = tok_ref[fs]
    pl.semaphore_wait(barrier, len(peers))

    sends = []
    for j, f in enumerate(others):
        copy = remote(tok_ref.at[f], blocks.at[tp, fs], a_send.at[j], a_recv.at[j], tp, f)
        copy.start()
        sends.append(copy)
    for j in range(n_stored - 1):
        sends[j].wait_recv()
    mid = []
    for j, d in enumerate(chips):
        copy = remote(blocks.at[tp], blocks.at[tp], b_send.at[j], b_recv.at[j],
                      2 * d + core, fs)
        copy.start()
        mid.append(copy)
    first = remote(blocks.at[tp], blocks.at[tp], c_send.at[0], c_recv.at[0], partner, fs)
    first.start()
    side = [first]
    for j, d in enumerate(chip_sources):
        mid[j].wait_recv()
        got = 2 * d + core
        copy = remote(blocks.at[got], blocks.at[got], c_send.at[j + 1], c_recv.at[j + 1],
                      partner, fs)
        copy.start()
        side.append(copy)
    for copy in side:
        copy.wait_recv()

    per = blocks.shape[1] * blocks.shape[2]
    cols = blocks.shape[3]
    group = 256 // pieces
    row_id = lax.broadcasted_iota(jnp.int32, (group, 256), 0)
    col_id = lax.broadcasted_iota(jnp.int32, (group, 256), 1)
    picks = [(col_id == row_id * pieces + q).astype(F32).astype(BF16) for q in range(pieces)]
    n_blocks = 256 // per
    for g in range(total // group):
        flat = blocks[g * n_blocks:(g + 1) * n_blocks].reshape(256, cols)
        for q in range(pieces):
            x[g * group:(g + 1) * group, q * cols:(q + 1) * cols] = jnp.dot(
                picks[q], flat, preferred_element_type=F32).astype(BF16)
    for copy in sends + mid + side:
        copy.wait_send()

    for i, copy in loads:
        if i < 2:
            copy.wait()

    rs = []
    for c, (at, size) in enumerate(chunks):
        for k, w in enumerate((gate_w, up_w)):
            value = jnp.dot(x[...], w[:, at:at + size], preferred_element_type=F32)
            if size < CHUNK:
                part[k] = jnp.zeros_like(part[k])
            part[k, :, :size] = value
            for f in range(n_stored):
                rs_send[c, f, k] = part[k, f * rows:(f + 1) * rows, :].astype(BF16)
            own[c, k] = part[k, pl.ds(pl.multiple_of(fs * rows, rows), rows), :]
        padded = min(CHUNK, round_up(size, LANES))
        copies = []
        for j, f in enumerate(others):
            copy = remote(rs_send.at[c, f, :, :, pl.ds(0, padded)],
                          rs_recv.at[c, fs, :, :, pl.ds(0, padded)],
                          rs_ssem.at[c, j], rs_rsem.at[c, j], tp, f)
            copy.start()
            copies.append(copy)
        rs.append(copies)

    def reduce(c):
        size = chunks[c][1]
        padded = min(CHUNK, round_up(size, LANES))
        gate, up = own[c, 0, :, :padded], own[c, 1, :, :padded]
        for j, f in enumerate(sources):
            rs[c][j].wait_recv()
            gate = gate + rs_recv[c, f, 0, :, :padded].astype(F32)
            up = up + rs_recv[c, f, 1, :, :padded].astype(F32)
        hid[c, fs, :, :padded] = (gate / (1.0 + jnp.exp(-gate)) * up).astype(BF16)
        copies = []
        for j, f in enumerate(others):
            copy = remote(hid.at[c, fs, :, pl.ds(0, padded)], hid.at[c, fs, :, pl.ds(0, padded)],
                          ag_ssem.at[c, j], ag_rsem.at[c, j], tp, f)
            copy.start()
            copies.append(copy)
        return copies

    def down(c, d):
        at, size = chunks[c]
        h = hid[c].reshape(total, CHUNK)[:, :size]
        return jnp.dot(h, down_w[at:at + size, d * 2 * lane_w:(d + 1) * 2 * lane_w],
                       preferred_element_type=F32)

    ag = []
    last = len(chunks) - 1
    for c in range(last + 1):
        ag.append(reduce(c))
    for i, copy in loads:
        if i == 2:
            copy.wait()
    pair = []
    for c in range(last + 1):
        for copy in ag[c]:
            copy.wait_recv()
        for d in range(n_chips):
            span = slice(d * 2 * lane_w, (d + 1) * 2 * lane_w)
            value = down(c, d)
            if c > 0:
                value = value + acc[:, span]
            if c < last:
                acc[:, span] = value
                continue
            low, high = value[:, :lane_w], value[:, lane_w:]
            keep[d] = jnp.where(core == 0, low, high)
            pair_send[d] = jnp.where(core == 0, high, low)
            copy = remote(pair_send.at[d], pair_recv.at[d], p_ssem.at[d], p_rsem.at[d],
                          partner, fs)
            copy.start()
            pair.append(copy)

    for d in range(n_chips):
        pair[d].wait_recv()
        value = keep[d] + pair_recv[d]
        keep[d] = value
        z_send[d] = value.astype(BF16)
    final = []
    for j, d in enumerate(chips):
        copy = remote(z_send.at[d], z_recv.at[chip], z_ssem.at[j], z_rsem.at[j],
                      2 * d + core, fs)
        copy.start()
        final.append(copy)
    value = keep[chip]
    for j, d in enumerate(chip_sources):
        final[j].wait_recv()
        value = value + z_recv[d].astype(F32)
    out_ref[...] = value.astype(BF16)

    for copy in [q for c in rs + ag for q in c] + pair + final:
        copy.wait_send()


def body(tokens, gate_weight, up_weight, down_weight):
    n_tensor, n_stored = lax.axis_size("tp"), lax.axis_size("fs")
    mine, model = tokens.shape
    depth, width = gate_weight.shape
    total = mine * n_tensor * n_stored
    pieces = max(1, SUBLANES // mine)
    cols = depth // pieces
    lane_w = depth // n_tensor
    n_chips = n_tensor // 2
    tok = tokens.reshape(mine, n_stored, pieces, cols).transpose(1, 0, 2, 3)
    tok = tok.reshape(n_stored, mine * pieces, cols)
    n_chunks = len(chunks_of(width))
    rows = total // n_stored
    dma = pltpu.SemaphoreType.DMA
    any_space = pl.BlockSpec(memory_space=pl.ANY)
    vmem = pl.BlockSpec(memory_space=pltpu.VMEM)
    return pl.pallas_call(
        functools.partial(kernel, n_tensor, n_stored, pieces),
        out_shape=jax.ShapeDtypeStruct((total, lane_w), BF16),
        in_specs=[vmem, any_space, any_space, any_space],
        out_specs=vmem,
        scratch_shapes=[
            pltpu.VMEM(gate_weight.shape, BF16),
            pltpu.VMEM(up_weight.shape, BF16),
            pltpu.VMEM(down_weight.shape, BF16),
            pltpu.VMEM((n_tensor, n_stored, mine * pieces, cols), BF16),
            pltpu.VMEM((total, depth), BF16),
            pltpu.VMEM((2, total, CHUNK), F32),
            pltpu.VMEM((n_chunks, 2, rows, CHUNK), F32),
            pltpu.VMEM((n_chunks, n_stored, 2, rows, CHUNK), BF16),
            pltpu.VMEM((n_chunks, n_stored, 2, rows, CHUNK), BF16),
            pltpu.VMEM((n_chunks, n_stored, rows, CHUNK), BF16),
            pltpu.VMEM((total, down_weight.shape[1]), F32),
            pltpu.VMEM((n_chips, total, lane_w), F32),
            pltpu.VMEM((n_chips, total, lane_w), F32),
            pltpu.VMEM((n_chips, total, lane_w), F32),
            pltpu.VMEM((n_chips, total, lane_w), BF16),
            pltpu.VMEM((n_chips, total, lane_w), BF16),
            dma((3, LOADS)),
            dma((n_stored,)), dma((n_stored,)),
            dma((n_chips,)), dma((n_chips,)),
            dma((n_chips,)), dma((n_chips,)),
            dma((n_chunks, n_stored)), dma((n_chunks, n_stored)),
            dma((n_chunks, n_stored)), dma((n_chunks, n_stored)),
            dma((n_chips,)), dma((n_chips,)),
            dma((n_chips,)), dma((n_chips,)),
        ],
        compiler_params=pltpu.CompilerParams(
            collective_id=0, has_side_effects=True, vmem_limit_bytes=62 * 2**20),
    )(tok, gate_weight, up_weight, down_weight)


def solution(mesh):
    return jax.shard_map(
        body,
        mesh=mesh,
        in_specs=(P(("tp", "fs"), None), P("fs", "tp"), P("fs", "tp"), P("tp", "fs")),
        out_specs=P(None, ("fs", "tp")),
        check_vma=False,
    )
```

```python
import functools

import jax
import jax.numpy as jnp
from jax import lax
from jax.experimental import pallas as pl
from jax.experimental.pallas import tpu as pltpu
from jax.sharding import PartitionSpec as P

BF16, F32 = jnp.bfloat16, jnp.float32
LANES, SUBLANES = 128, 16
CHUNK = 5 * LANES


def chunks_of(width):
    out, at = [], 0
    for size in (256, 512):
        if at + size < width:
            out.append((at, size))
            at += size
    return out + [(q, min(CHUNK, width - q)) for q in range(at, width, CHUNK)]


def round_up(n, m):
    return (n + m - 1) // m * m


def kernel(n_tensor, n_stored, pieces, tok_ref, gate_hbm, up_hbm, down_hbm, out_ref,
           gate_w, up_w, down_w, blocks, x, part, own, rs_send, rs_recv, hid,
           acc, keep, pair_send, pair_recv, z_send, z_recv,
           load_sem, a_send, a_recv, b_send, b_recv, c_send, c_recv,
           rs_ssem, rs_rsem, ag_ssem, ag_rsem, p_ssem, p_rsem, z_ssem, z_rsem):
    tp, fs = lax.axis_index("tp"), lax.axis_index("fs")
    core, chip = lax.rem(tp, 2), tp // 2
    partner = tp + 1 - 2 * core
    n_chips = n_tensor // 2
    width = gate_w.shape[0]
    chunks = chunks_of(width)
    total = x.shape[0]
    lane_w = keep.shape[2]

    loads = {}
    for i, (hbm, vmem) in enumerate(((gate_hbm, gate_w), (up_hbm, up_w), (down_hbm, down_w))):
        for c, (at, size) in enumerate(chunks):
            span = pl.ds(at, size)
            loads[i, c] = pltpu.make_async_copy(
                hbm.at[span, :], vmem.at[span, :], load_sem.at[i, c])
    for c in range(len(chunks)):
        loads[0, c].start()
        loads[1, c].start()
    for c in range(len(chunks)):
        loads[2, c].start()

    def remote(src, dst, ssem, rsem, tensor, stored):
        return pltpu.make_async_remote_copy(
            src_ref=src, dst_ref=dst, send_sem=ssem, recv_sem=rsem,
            device_id={"tp": tensor, "fs": stored},
            device_id_type=pl.DeviceIdType.MESH)

    others = [lax.rem(fs + j, n_stored) for j in range(1, n_stored)]
    sources = [lax.rem(fs + n_stored - j, n_stored) for j in range(1, n_stored)]
    chips = [lax.rem(chip + j, n_chips) for j in range(1, n_chips)]
    chip_sources = [lax.rem(chip + n_chips - j, n_chips) for j in range(1, n_chips)]

    barrier = pltpu.get_barrier_semaphore()
    peers = [(tp, f) for f in others] + [(2 * d + core, fs) for d in chips] + [(partner, fs)]
    for tensor, stored in peers:
        pl.semaphore_signal(barrier, inc=1, device_id={"tp": tensor, "fs": stored},
                            device_id_type=pl.DeviceIdType.MESH)
    blocks[tp, fs] = tok_ref[fs]
    pl.semaphore_wait(barrier, len(peers))

    sends = []
    for j, f in enumerate(others):
        copy = remote(tok_ref.at[f], blocks.at[tp, fs], a_send.at[j], a_recv.at[j], tp, f)
        copy.start()
        sends.append(copy)
    for j in range(n_stored - 1):
        sends[j].wait_recv()
    mid = []
    for j, d in enumerate(chips):
        copy = remote(blocks.at[tp], blocks.at[tp], b_send.at[j], b_recv.at[j],
                      2 * d + core, fs)
        copy.start()
        mid.append(copy)
    first = remote(blocks.at[tp], blocks.at[tp], c_send.at[0], c_recv.at[0], partner, fs)
    first.start()
    side = [first]
    for j, d in enumerate(chip_sources):
        mid[j].wait_recv()
        got = 2 * d + core
        copy = remote(blocks.at[got], blocks.at[got], c_send.at[j + 1], c_recv.at[j + 1],
                      partner, fs)
        copy.start()
        side.append(copy)
    for copy in side:
        copy.wait_recv()

    per = blocks.shape[1] * blocks.shape[2]
    cols = blocks.shape[3]
    group = 256 // pieces
    row_id = lax.broadcasted_iota(jnp.int32, (group, 256), 0)
    col_id = lax.broadcasted_iota(jnp.int32, (group, 256), 1)
    picks = [(col_id == row_id * pieces + q).astype(F32).astype(BF16) for q in range(pieces)]
    n_blocks = 256 // per
    for g in range(total // group):
        flat = blocks[g * n_blocks:(g + 1) * n_blocks].reshape(256, cols)
        for q in range(pieces):
            x[g * group:(g + 1) * group, q * cols:(q + 1) * cols] = jnp.dot(
                picks[q], flat, preferred_element_type=F32).astype(BF16)
    for copy in sends + mid + side:
        copy.wait_send()

    def share(c):
        return round_up(chunks[c][1], SUBLANES * n_stored) // n_stored

    rs = []
    for c, (at, size) in enumerate(chunks):
        sub = share(c)
        for k, w in enumerate((gate_w, up_w)):
            loads[k, c].wait()
            part[k, :size, :] = lax.dot_general(
                w[at:at + size, :], x[...], (((1,), (1,)), ((), ())),
                preferred_element_type=F32)
            if size < sub * n_stored:
                part[k, size:sub * n_stored, :] = jnp.zeros((sub * n_stored - size, total), F32)
            for f in range(n_stored):
                rs_send[c, f, k, :sub, :] = part[k, f * sub:(f + 1) * sub, :].astype(BF16)
            own[c, k, :sub, :] = part[k, pl.ds(pl.multiple_of(fs * sub, sub), sub), :]
        copies = []
        for j, f in enumerate(others):
            copy = remote(rs_send.at[c, f, :, pl.ds(0, sub), :],
                          rs_recv.at[c, fs, :, pl.ds(0, sub), :],
                          rs_ssem.at[c, j], rs_rsem.at[c, j], tp, f)
            copy.start()
            copies.append(copy)
        rs.append(copies)

    def reduce(c):
        sub = share(c)
        gate, up = own[c, 0, :sub, :], own[c, 1, :sub, :]
        for j, f in enumerate(sources):
            rs[c][j].wait_recv()
            gate = gate + rs_recv[c, f, 0, :sub, :].astype(F32)
            up = up + rs_recv[c, f, 1, :sub, :].astype(F32)
        hid[c, fs, :sub, :] = (gate / (1.0 + jnp.exp(-gate)) * up).astype(BF16)
        copies = []
        for j, f in enumerate(others):
            copy = remote(hid.at[c, fs, pl.ds(0, sub), :], hid.at[c, fs, pl.ds(0, sub), :],
                          ag_ssem.at[c, j], ag_rsem.at[c, j], tp, f)
            copy.start()
            copies.append(copy)
        return copies

    def down(c, d):
        at, size = chunks[c]
        sub = share(c)
        h = hid[c, :, :sub, :].reshape(n_stored * sub, total)[:size]
        w = down_w[at:at + size, d * 2 * lane_w:(d + 1) * 2 * lane_w]
        return lax.dot_general(h, w, (((0,), (0,)), ((), ())), preferred_element_type=F32)

    ag = []
    last = len(chunks) - 1
    for c in range(last + 1):
        ag.append(reduce(c))
    pair = []
    for c in range(last + 1):
        loads[2, c].wait()
        for copy in ag[c]:
            copy.wait_recv()
        for d in range(n_chips):
            span = slice(d * 2 * lane_w, (d + 1) * 2 * lane_w)
            value = down(c, d)
            if c > 0:
                value = value + acc[:, span]
            if c < last:
                acc[:, span] = value
                continue
            low, high = value[:, :lane_w], value[:, lane_w:]
            keep[d] = jnp.where(core == 0, low, high)
            pair_send[d] = jnp.where(core == 0, high, low)
            copy = remote(pair_send.at[d], pair_recv.at[d], p_ssem.at[d], p_rsem.at[d],
                          partner, fs)
            copy.start()
            pair.append(copy)

    for d in range(n_chips):
        pair[d].wait_recv()
        value = keep[d] + pair_recv[d]
        keep[d] = value
        z_send[d] = value.astype(BF16)
    final = []
    for j, d in enumerate(chips):
        copy = remote(z_send.at[d], z_recv.at[chip], z_ssem.at[j], z_rsem.at[j],
                      2 * d + core, fs)
        copy.start()
        final.append(copy)
    value = keep[chip]
    for j, d in enumerate(chip_sources):
        final[j].wait_recv()
        value = value + z_recv[d].astype(F32)
    out_ref[...] = value.astype(BF16)

    for copy in [q for c in rs + ag for q in c] + pair + final:
        copy.wait_send()


def body(tokens, gate_weight, up_weight, down_weight):
    n_tensor, n_stored = lax.axis_size("tp"), lax.axis_size("fs")
    mine, model = tokens.shape
    depth, width = gate_weight.shape
    total = mine * n_tensor * n_stored
    pieces = max(1, SUBLANES // mine)
    cols = depth // pieces
    lane_w = depth // n_tensor
    n_chips = n_tensor // 2
    tok = tokens.reshape(mine, n_stored, pieces, cols).transpose(1, 0, 2, 3)
    tok = tok.reshape(n_stored, mine * pieces, cols)
    n_chunks = len(chunks_of(width))
    most = CHUNK // n_stored
    dma = pltpu.SemaphoreType.DMA
    any_space = pl.BlockSpec(memory_space=pl.ANY)
    vmem = pl.BlockSpec(memory_space=pltpu.VMEM)
    return pl.pallas_call(
        functools.partial(kernel, n_tensor, n_stored, pieces),
        out_shape=jax.ShapeDtypeStruct((total, lane_w), BF16),
        in_specs=[vmem, any_space, any_space, any_space],
        out_specs=vmem,
        scratch_shapes=[
            pltpu.VMEM((width, depth), BF16),
            pltpu.VMEM((width, depth), BF16),
            pltpu.VMEM(down_weight.shape, BF16),
            pltpu.VMEM((n_tensor, n_stored, mine * pieces, cols), BF16),
            pltpu.VMEM((total, depth), BF16),
            pltpu.VMEM((2, CHUNK, total), F32),
            pltpu.VMEM((n_chunks, 2, most, total), F32),
            pltpu.VMEM((n_chunks, n_stored, 2, most, total), BF16),
            pltpu.VMEM((n_chunks, n_stored, 2, most, total), BF16),
            pltpu.VMEM((n_chunks, n_stored, most, total), BF16),
            pltpu.VMEM((total, down_weight.shape[1]), F32),
            pltpu.VMEM((n_chips, total, lane_w), F32),
            pltpu.VMEM((n_chips, total, lane_w), F32),
            pltpu.VMEM((n_chips, total, lane_w), F32),
            pltpu.VMEM((n_chips, total, lane_w), BF16),
            pltpu.VMEM((n_chips, total, lane_w), BF16),
            dma((3, n_chunks)),
            dma((n_stored,)), dma((n_stored,)),
            dma((n_chips,)), dma((n_chips,)),
            dma((n_chips,)), dma((n_chips,)),
            dma((n_chunks, n_stored)), dma((n_chunks, n_stored)),
            dma((n_chunks, n_stored)), dma((n_chunks, n_stored)),
            dma((n_chips,)), dma((n_chips,)),
            dma((n_chips,)), dma((n_chips,)),
        ],
        compiler_params=pltpu.CompilerParams(
            collective_id=0, has_side_effects=True, vmem_limit_bytes=62 * 2**20),
    )(tok, gate_weight.T, up_weight.T, down_weight)


def solution(mesh):
    return jax.shard_map(
        body,
        mesh=mesh,
        in_specs=(P(("tp", "fs"), None), P("fs", "tp"), P("fs", "tp"), P("tp", "fs")),
        out_specs=P(None, ("fs", "tp")),
        check_vma=False,
    )
```
